32 devices in a mesh: groups: 2 (over x), ep: 8 (over z, y), rep: 2 (over core).
Axes of the slice: x: 2, y: 2, z: 4, core: 2. Of those that a mesh axis runs over, the one named last changes fastest.
Arguments:
- tokens: bfloat16 [512, 3584], P(('groups', 'ep'), 'rep'), parts along dimension 0, may hold values from -6 to 6
- expert_ids: int32 [512, 1], P(('groups', 'ep')), parts along dimension 0, may hold values from 0 to 3; in each aligned block of 32 rows (0 to 31, 32 to 63, ...) at most 10 rows name the same one
- gate_values: float32 [512, 1], P(('groups', 'ep')), parts along dimension 0, may hold values from 0.1 to 0.6
- slot_expert: int32 [8], replicated, may hold values from 0 to 3, as said below
- gate_weight: bfloat16 [8, 3584, 1024], P('ep', None, 'rep'), as said below
- up_weight: bfloat16 [8, 3584, 1024], P('ep', None, 'rep'), as said below
- down_weight: bfloat16 [8, 1024, 3584], P('ep', 'rep'), as said below
Outputs:
- combined: bfloat16 [512, 3584], P(('groups', 'ep'), 'rep'), parts along dimension 0
The draws below stay inside these ranges and needn't reach their ends.
There are 2 independent parts, one for each index of `groups`. The reference program is written for one: setup_inputs(seed, part) draws one part's arguments, and reference() takes and returns one part's arrays. A program takes and returns all parts, laid end to end along the dimension named above; an argument that names none is the same for every part. Nothing has to cross between parts.
Inputs may be any that keep to these rules, and one draw needn't show every extreme that they name: `expert_ids`: each row names 1 different experts. Among the 32 rows of one index of ep (aligned blocks) no expert is named more than 10 times, and in some blocks one expert is named exactly 10 times. `slot_expert`: every expert is held by 1 to 4 slots, and some experts by 4. gate_weight[s] equals gate_weight[r] whenever slot_expert[s] equals slot_expert[r]. up_weight[s] equals up_weight[r] whenever slot_expert[s] equals slot_expert[r]. down_weight[s] equals down_weight[r] whenever slot_expert[s] equals slot_expert[r].
All inputs are finite; a program needn't handle non-finite values.
Results may differ from the reference program's by a relative error of at most 0.0057.
Values may be sent and summed in bfloat16 or wider, within the bound.
A program may use at most 128 MiB of HBM per device.

```python
import math
import jax
import jax.numpy as jnp
import numpy as np
from jax import lax

D = 3584
HID = 1024
TOK_EP = 32
EXPERTS = 4
TOP = 1
CAP = 10
TOKENS = 256
N_EP = 8


def plan_of(key):
    plan_key = jax.random.fold_in(key, 11)
    first_key, second_key = jax.random.split(plan_key)
    ordering = jax.random.permutation(first_key, EXPERTS)
    ranked = jnp.arange(EXPERTS)
    quarter = EXPERTS // 4
    copies = jnp.where(ranked < quarter, 4, jnp.where(ranked < 2 * quarter, 2, 1))
    listing = jnp.repeat(ordering, copies, total_repeat_length=2 * EXPERTS)
    shuffle = jax.random.permutation(second_key, 2 * EXPERTS)
    return listing[shuffle].astype(jnp.int32)


def slot_weights(key, salt_value, row_count, col_count):
    holders = plan_of(key)
    weight_key = jax.random.fold_in(key, salt_value)
    spread = 1.0 / math.sqrt(row_count)

    def one_slot(expert):
        return jax.random.normal(jax.random.fold_in(weight_key, expert), (row_count, col_count), jnp.float32) * spread
    return jax.vmap(one_slot)(holders)


def draw_slot_expert(key, part):
    return plan_of(key)


def draw_gate_weight(key, part):
    return slot_weights(key, 21, D, HID).astype(jnp.bfloat16)


def draw_up_weight(key, part):
    return slot_weights(key, 22, D, HID).astype(jnp.bfloat16)


def draw_down_weight(key, part):
    return slot_weights(key, 23, HID, D).astype(jnp.bfloat16)


def steps_of(rng, extent, cuts, least, largest):
    gain, own = 1.0, jax.random.fold_in(rng, 6)
    for dim, blocks in cuts:
        heights = jnp.exp(jax.random.uniform(jax.random.fold_in(own, dim), (blocks,), jnp.float32, least / len(cuts), largest / len(cuts)))
        gain = gain * jnp.repeat(heights, extent[dim] // blocks).reshape([-1 if axis == dim else 1 for axis in range(len(extent))])
    return gain


def assign_block(own_key, own, number, rows, number_of, top, limit, skew):
    sequence = jax.random.permutation(own_key, number_of)
    packed, usual = load_shares(number_of, rows * top, limit, skew, True), load_shares(number_of, rows * top, limit, skew, False)
    places = jnp.arange(number_of)

    def named(tallies, rotation):
        used = int((tallies > 0).sum())
        fixed = max(1, used // 4)
        passed = fixed + (places - fixed + rotation * (used - fixed)) % max(1, number_of - fixed)
        return jnp.zeros((number_of,), jnp.int32).at[sequence[jnp.where(places < fixed, places, passed)]].set(jnp.asarray(tallies, jnp.int32))

    tallies = jnp.where(number % 4 == 0, named(packed, number // 4), named(usual, number - number // 4 - 1))
    mixed = jax.random.permutation(jax.random.fold_in(own, 3), number_of)
    giver, receiver = mixed[0:number_of // 2 * 2:2], mixed[1:number_of // 2 * 2:2]
    margin = jnp.minimum(tallies[giver] - 1, limit - tallies[receiver]) // 2
    margin = jnp.where((giver == sequence[0]) | (receiver == sequence[0]) | (tallies[receiver] == 0), 0, jnp.maximum(margin, 0))
    passed = jax.random.randint(jax.random.fold_in(own, 4), (number_of // 2,), 0, 1 << 20) % (margin + 1)
    tallies = tallies.at[giver].add(-passed).at[receiver].add(passed)
    items = jnp.searchsorted(jnp.cumsum(tallies), jnp.arange(rows * top), side="right").astype(jnp.int32)
    table = items.reshape(top, rows).T
    table = table[jax.random.permutation(jax.random.fold_in(own, 1), rows)]
    rotation = jax.random.randint(jax.random.fold_in(own, 2), (rows, 1), 0, top)
    return jnp.take_along_axis(table, (jnp.arange(top)[None, :] + rotation) % top, axis=1)


def load_shares(number_of, total, reach, skew, full):
    loads = [(1 << 20) // math.isqrt(grade ** skew) + 1 for grade in range(1, number_of + 1)]
    largest = reach if full else min(reach, max(-(-total // number_of), total * loads[0] // sum(loads)))
    least = 1 if total - largest >= number_of - 1 else 0
    counts, rest = [largest] + [least] * (number_of - 1), total - largest - least * (number_of - 1)
    while rest > 0:
        movable = [i for i in range(1, number_of) if counts[i] < largest] or [i for i in range(1, number_of) if counts[i] < reach]
        mass, budget = sum([loads[i] for i in movable]), rest
        for i in movable:
            addition = min(reach - counts[i], max(1, budget * loads[i] // mass), rest)
            counts[i] = counts[i] + addition
            rest = rest - addition
    return np.array(counts)


def scatter_about(key, dims, deviation, reach, pieces=(), held_as=jnp.bfloat16):
    drawn = jax.random.normal(key, dims, jnp.float32) * deviation
    if len(pieces) > 0:
        drawn = steps_of(key, dims, pieces, -0.22, 0.18) * drawn
    return jnp.clip(drawn, min=-reach, max=reach).astype(held_as)


def setup_inputs(seed: int = 0, part: int = 0) -> dict:
    seeds = jax.random.split(jax.random.key(seed), 8)
    own_keys = jax.random.split(jax.random.fold_in(seeds[7], part), 8)
    tokens = scatter_about(own_keys[0], (TOKENS, D), 1.0, 6.0, ((0, 8), (1, 2)))
    expert_ids_keys = jax.random.split(jax.random.fold_in(own_keys[1], 1), TOKENS // TOK_EP)
    expert_ids_turns = jax.random.permutation(jax.random.fold_in(own_keys[1], 3), TOKENS // TOK_EP)
    expert_ids = jax.vmap(lambda own, number: assign_block(jax.random.fold_in(own_keys[1], 2), own, number, TOK_EP, EXPERTS, TOP, CAP, 2))(expert_ids_keys, expert_ids_turns).reshape((TOKENS, TOP))
    gate_values = jnp.clip(0.1 + 0.5 * jax.random.uniform(own_keys[2], (TOKENS, TOP), jnp.float32) ** steps_of(own_keys[2], (TOKENS, TOP), ((0, 8),), -0.2, 0.2), 0.1, 0.6)
    slot_expert = draw_slot_expert(jax.random.fold_in(seeds[7], 71), part)
    gate_weight = draw_gate_weight(jax.random.fold_in(seeds[7], 71), part)
    up_weight = draw_up_weight(jax.random.fold_in(seeds[7], 71), part)
    down_weight = draw_down_weight(jax.random.fold_in(seeds[7], 71), part)
    return {"tokens": tokens, "expert_ids": expert_ids, "gate_values": gate_values, "slot_expert": slot_expert, "gate_weight": gate_weight, "up_weight": up_weight, "down_weight": down_weight}


def reference(tokens, expert_ids, gate_values, slot_expert, gate_weight, up_weight, down_weight):
    pair_count = TOKENS * TOP
    row_bound = min(pair_count, N_EP * CAP)
    pair_expert = expert_ids.reshape(pair_count)
    padded = jnp.concatenate([tokens, jnp.zeros((1, D), tokens.dtype)], axis=0)
    flat_gates = jnp.concatenate([gate_values.reshape(pair_count), jnp.zeros((1,), gate_values.dtype)], axis=0)

    def one_expert(running, expert):
        slot_index = jnp.argmax(slot_expert == expert).astype(jnp.int32)
        members = jnp.nonzero(pair_expert == expert, size=row_bound, fill_value=pair_count)[0].astype(jnp.int32)
        row_block = padded[members // TOP]
        gate_proj = jnp.dot(row_block, gate_weight[slot_index], preferred_element_type=jnp.float32)
        up_proj = jnp.dot(row_block, up_weight[slot_index], preferred_element_type=jnp.float32)
        hidden = (jax.nn.silu(gate_proj) * up_proj).astype(jnp.bfloat16)
        outcome = jnp.dot(hidden, down_weight[slot_index], preferred_element_type=jnp.float32).astype(jnp.bfloat16)
        weight = flat_gates[members]
        running = running.at[members // TOP].add(weight[:, None] * outcome.astype(jnp.float32))
        return running, None

    running, _ = lax.scan(one_expert, jnp.zeros((TOKENS + 1, D), jnp.float32), jnp.arange(EXPERTS, dtype=jnp.int32))
    return running[:TOKENS].astype(jnp.bfloat16)
```

```python
import functools

import jax
import jax.numpy as jnp
from jax import lax
from jax.experimental import pallas as pl
from jax.experimental.pallas import tpu as pltpu
from jax.sharding import PartitionSpec as P

MESH = pl.DeviceIdType.MESH
F32 = jnp.float32
BF16 = jnp.bfloat16
HEAD = 8


def iota(shape, dim):
    return lax.broadcasted_iota(jnp.int32, shape, dim)


def repeat(count, step):
    if count <= 8:
        for i in range(count):
            step(i)
    else:
        lax.fori_loop(0, count, lambda i, c: (step(i), c)[1], 0)


def routing(ids, slots_row, ep, head, tail):
    top, rows = ids.shape
    n = slots_row.shape[1]
    at_row, at_col = iota((n, n), 0), iota((n, n), 1)
    slots_all = jnp.broadcast_to(slots_row, (n, n))
    slots_col = jnp.sum(jnp.where(at_row == at_col, slots_all, 0), axis=1, keepdims=True)
    same = slots_col == slots_all
    copies = jnp.sum(jnp.where(same, 1, 0), axis=1, keepdims=True)
    rank = jnp.sum(jnp.where(same & (at_col < at_row), 1, 0), axis=1, keepdims=True)
    want = jnp.zeros_like(copies)
    for c in range(2, 5):
        want = jnp.where(copies == c, lax.rem(ep, c), want)
    goes = jnp.zeros((n, rows), F32)
    for k in range(top):
        hit = (ids[k : k + 1, :] == slots_col) & (rank == want)
        goes = jnp.where(hit, 1.0, goes)
    before = jnp.where(iota((rows, rows), 0) < iota((rows, rows), 1), 1.0, 0.0)
    place = jnp.dot(goes, before, preferred_element_type=F32)
    out = []
    for first, size in ((0, head), (head, tail)):
        if size == 0:
            out.append(None)
            continue
        r, s = iota((n * size, n), 0), iota((n * size, n), 1)
        mine = (r >= s * size) & (r < s * size + size)
        spread = jnp.where(mine, 1.0, 0.0)
        rank_in = jnp.sum(jnp.where(mine, r - s * size + first, 0), axis=1, keepdims=True)
        experts = jnp.sum(
            jnp.where(mine, jnp.broadcast_to(slots_row, (n * size, n)), 0), axis=1, keepdims=True
        )
        goes_r = jnp.dot(spread, goes, preferred_element_type=F32)
        place_r = jnp.dot(spread, place, preferred_element_type=F32)
        chosen = (goes_r > 0.5) & (place_r == rank_in.astype(F32))
        out.append((jnp.where(chosen, 1.0, 0.0), experts))
    return out


def kernel(n, cap, tok, ids_ref, slots_ref, gates_ref, wg_hbm, wu_hbm, wd_hbm, out_ref,
           wg, wu, wd, send_a, send_b, x_a, x_b, hid, acc, res_a, res_b, ret_a, ret_b,
           w_sem, d_send, d_recv, s_send, s_recv, f_send, f_recv, h_send, h_recv, r_send, r_recv):
    ep, rep = lax.axis_index("ep"), lax.axis_index("rep")
    other = 1 - rep
    rows, half = tok.shape
    tail = cap - HEAD
    hidden = hid.shape[2]

    barrier = pltpu.get_barrier_semaphore()

    def greet(d):
        pl.semaphore_signal(barrier, inc=1, device_id={"ep": lax.rem(ep + 1 + d, n)}, device_id_type=MESH)

    repeat(n - 1, greet)
    pl.semaphore_signal(barrier, inc=1, device_id={"rep": other}, device_id_type=MESH)

    weights = [
        pltpu.make_async_copy(wg_hbm.at[0], wg, w_sem.at[0]),
        pltpu.make_async_copy(wu_hbm.at[0], wu, w_sem.at[1]),
        pltpu.make_async_copy(
            wd_hbm.at[0, :, pl.ds(pl.multiple_of(rep * half, 128), half)], wd.at[rep], w_sem.at[2]
        ),
    ]
    for copy in weights:
        copy.start()

    (pick_a, _), picked_b = routing(ids_ref[...], slots_ref[...], ep, HEAD, tail)
    tokens = tok[...]
    packed = jnp.dot(pick_a.astype(BF16), tokens, preferred_element_type=F32).astype(BF16)
    send_a[...] = packed.reshape(n, HEAD, half)
    packed = jnp.dot(picked_b[0].astype(BF16), tokens, preferred_element_type=F32)
    for s in range(n):
        send_b[s] = packed[s * tail : s * tail + tail].astype(BF16)

    pl.semaphore_wait(barrier, n)

    down = pltpu.make_async_remote_copy(
        src_ref=wd_hbm.at[0, :, pl.ds(pl.multiple_of(other * half, 128), half)],
        dst_ref=wd.at[rep], send_sem=d_send, recv_sem=d_recv,
        device_id={"rep": other}, device_id_type=MESH,
    )
    down_in = pltpu.make_async_remote_copy(
        src_ref=wd_hbm.at[0, :, pl.ds(pl.multiple_of(other * half, 128), half)],
        dst_ref=wd.at[other], send_sem=d_send, recv_sem=d_recv,
        device_id={"rep": other}, device_id_type=MESH,
    )

    def packet(target, origin, part):
        src, dst = ((send_a, x_a), (send_b, x_b))[part]
        return pltpu.make_async_remote_copy(
            src_ref=src.at[target], dst_ref=dst.at[rep, origin],
            send_sem=s_send.at[part, target], recv_sem=s_recv.at[part, origin],
            device_id={"ep": target}, device_id_type=MESH,
        )

    def forward(origin, part, side):
        dst = (x_a, x_b)[part]
        return pltpu.make_async_remote_copy(
            src_ref=dst.at[side, origin], dst_ref=dst.at[side, origin],
            send_sem=f_send.at[part, origin], recv_sem=f_recv.at[part, origin],
            device_id={"rep": other}, device_id_type=MESH,
        )

    def back(target, origin, part):
        src, dst = ((res_a, ret_a), (res_b, ret_b))[part]
        return pltpu.make_async_remote_copy(
            src_ref=src.at[target], dst_ref=dst.at[origin],
            send_sem=r_send.at[part, target], recv_sem=r_recv.at[part, origin],
            device_id={"ep": target}, device_id_type=MESH,
        )

    def start_packets(d):
        to = lax.rem(ep + 1 + d, n)
        for part in range(2):
            packet(to, ep, part).start()

    repeat(n - 1, start_packets)
    down.start()
    x_a[rep, ep] = send_a[ep]
    x_b[rep, ep] = send_b[ep]
    for part in range(2):
        forward(ep, part, rep).start()

    def pass_on(d):
        origin = lax.rem(ep + n - 1 - d, n)
        for part in range(2):
            packet(origin, origin, part).wait_recv()
            forward(origin, part, rep).start()

    repeat(n - 1, pass_on)
    for copy in weights[:2]:
        copy.wait()

    def block(side):
        lower = x_b[side].reshape(n * tail, half)
        return jnp.concatenate([x_a[side].reshape(n * HEAD, half), lower], axis=0)

    mine = pl.ds(pl.multiple_of(rep * half, 16), half)
    theirs = pl.ds(pl.multiple_of(other * half, 16), half)
    x_mine = block(rep)
    gate = jnp.dot(x_mine, wg[mine, :], preferred_element_type=F32)
    up = jnp.dot(x_mine, wu[mine, :], preferred_element_type=F32)

    def arrive(j):
        for part in range(2):
            forward(j, part, other).wait_recv()

    repeat(n, arrive)
    x_theirs = block(other)
    gate = gate + jnp.dot(x_theirs, wg[theirs, :], preferred_element_type=F32)
    up = up + jnp.dot(x_theirs, wu[theirs, :], preferred_element_type=F32)
    hid[rep] = ((gate / (1.0 + jnp.exp(-gate))) * up).astype(BF16)

    def share(side):
        return pltpu.make_async_remote_copy(
            src_ref=hid.at[side], dst_ref=hid.at[side], send_sem=h_send, recv_sem=h_recv,
            device_id={"rep": other}, device_id_type=MESH,
        )

    share(rep).start()
    weights[2].wait()
    acc[...] = jnp.dot(hid[rep], wd[rep], preferred_element_type=F32)
    down_in.wait_recv()
    share(other).wait_recv()
    result = acc[...] + jnp.dot(hid[other], wd[other], preferred_element_type=F32)
    res_a[...] = result[: n * HEAD].astype(BF16).reshape(n, HEAD, half)
    for s in range(n):
        lo = n * HEAD + s * tail
        res_b[s] = result[lo : lo + tail].astype(BF16)

    def start_back(d):
        to = lax.rem(ep + 1 + d, n)
        for part in range(2):
            back(to, ep, part).start()

    repeat(n - 1, start_back)
    ret_a[ep] = res_a[ep]
    ret_b[ep] = res_b[ep]

    down.wait_send()
    share(rep).wait_send()

    def sent(d):
        to = lax.rem(ep + 1 + d, n)
        for part in range(2):
            packet(to, ep, part).wait_send()
            forward(to, part, rep).wait_send()

    repeat(n - 1, sent)
    for part in range(2):
        forward(ep, part, rep).wait_send()

    def came_back(d):
        origin = lax.rem(ep + n - 1 - d, n)
        for part in range(2):
            back(origin, origin, part).wait_recv()

    repeat(n - 1, came_back)

    ids = ids_ref[...]
    gates = gates_ref[...]
    top = ids.shape[0]
    (pick_a, exp_a), (pick_b, exp_b) = routing(ids, slots_ref[...], ep, HEAD, tail)
    all_a = ret_a[...].reshape(n * HEAD, half)
    all_b = ret_b[...].reshape(n * tail, half)
    over = (((0,), (0,)), ((), ()))
    diagonal = iota((rows, rows), 0) == iota((rows, rows), 1)
    total = None
    for k in range(top):
        hit_a = jnp.where(ids[k : k + 1, :] == exp_a, pick_a, 0.0).astype(BF16)
        hit_b = jnp.where(ids[k : k + 1, :] == exp_b, pick_b, 0.0).astype(BF16)
        got = lax.dot_general(hit_a, all_a, over, preferred_element_type=F32)
        got = got + lax.dot_general(hit_b, all_b, over, preferred_element_type=F32)
        line = jnp.broadcast_to(gates[k : k + 1, :], (rows, rows))
        column = jnp.sum(jnp.where(diagonal, line, 0.0), axis=1, keepdims=True)
        total = got * column if total is None else total + got * column
    out_ref[...] = total.astype(BF16)

    def back_sent(d):
        to = lax.rem(ep + 1 + d, n)
        for part in range(2):
            back(to, ep, part).wait_send()

    repeat(n - 1, back_sent)


def body(tokens, expert_ids, gate_values, slot_expert, gate_weight, up_weight, down_weight):
    rows, top = expert_ids.shape
    half = tokens.shape[1]
    n = slot_expert.shape[0]
    experts = n // 2
    cap = rows * top * 5 // (4 * experts)
    tail = cap - HEAD
    depth, hidden = gate_weight.shape[1:]
    vmem = pl.BlockSpec(memory_space=pltpu.VMEM)
    hbm = pl.BlockSpec(memory_space=pl.ANY)
    dma = pltpu.SemaphoreType.DMA
    return pl.pallas_call(
        functools.partial(kernel, n, cap),
        out_shape=jax.ShapeDtypeStruct((rows, half), BF16),
        in_specs=[vmem] * 4 + [hbm] * 3,
        out_specs=vmem,
        scratch_shapes=[
            pltpu.VMEM((depth, hidden), BF16),
            pltpu.VMEM((depth, hidden), BF16),
            pltpu.VMEM((2, hidden, half), BF16),
            pltpu.VMEM((n, HEAD, half), BF16),
            pltpu.VMEM((n, tail, half), BF16),
            pltpu.VMEM((2, n, HEAD, half), BF16),
            pltpu.VMEM((2, n, tail, half), BF16),
            pltpu.VMEM((2, n * cap, hidden), BF16),
            pltpu.VMEM((n * cap, half), F32),
            pltpu.VMEM((n, HEAD, half), BF16),
            pltpu.VMEM((n, tail, half), BF16),
            pltpu.VMEM((n, HEAD, half), BF16),
            pltpu.VMEM((n, tail, half), BF16),
            dma((3,)),
            dma, dma,
            dma((2, n)), dma((2, n)),
            dma((2, n)), dma((2, n)),
            dma, dma,
            dma((2, n)), dma((2, n)),
        ],
        compiler_params=pltpu.CompilerParams(
            collective_id=0, has_side_effects=True, vmem_limit_bytes=60000 * 1024
        ),
    )(tokens, expert_ids.T, slot_expert.reshape(1, n), gate_values.T,
      gate_weight, up_weight, down_weight)


def solution(mesh):
    return jax.shard_map(
        body,
        mesh=mesh,
        in_specs=(
            P(("groups", "ep"), "rep"),
            P(("groups", "ep"), None),
            P(("groups", "ep"), None),
            P(),
            P("ep", None, "rep"),
            P("ep", None, "rep"),
            P("ep", "rep", None),
        ),
        out_specs=P(("groups", "ep"), "rep"),
        check_vma=False,
    )
```

```python
import functools

import jax
import jax.numpy as jnp
from jax import lax
from jax.experimental import pallas as pl
from jax.experimental.pallas import tpu as pltpu
from jax.sharding import PartitionSpec as P

MESH = pl.DeviceIdType.MESH
F32 = jnp.float32
BF16 = jnp.bfloat16
HEAD = 8


def iota(shape, dim):
    return lax.broadcasted_iota(jnp.int32, shape, dim)


def repeat(low, high, step):
    if high - low <= 8:
        for i in reversed(range(low, high)):
            step(i)
    else:
        lax.fori_loop(0, high - low, lambda i, c: (step(high - 1 - i), c)[1], 0)


def mix(n, a, b):
    total, bit = 0, 1
    while bit < n:
        total = total + (a // bit + b // bit) % 2 * bit
        bit *= 2
    return total


def routing(ids, slots_row, ep, head, tail):
    top, rows = ids.shape
    n = slots_row.shape[1]
    at_row, at_col = iota((n, n), 0), iota((n, n), 1)
    slots_all = jnp.broadcast_to(slots_row, (n, n))
    slots_col = jnp.sum(jnp.where(at_row == at_col, slots_all, 0), axis=1, keepdims=True)
    same = slots_col == slots_all
    copies = jnp.sum(jnp.where(same, 1, 0), axis=1, keepdims=True)
    rank = jnp.sum(jnp.where(same & (at_col < at_row), 1, 0), axis=1, keepdims=True)
    want = jnp.zeros_like(copies)
    for c in range(2, 5):
        want = jnp.where(copies == c, lax.rem(ep, c), want)
    goes = jnp.zeros((n, rows), F32)
    for k in range(top):
        hit = (ids[k : k + 1, :] == slots_col) & (rank == want)
        goes = jnp.where(hit, 1.0, goes)
    before = jnp.where(iota((rows, rows), 0) < iota((rows, rows), 1), 1.0, 0.0)
    place = jnp.dot(goes, before, preferred_element_type=F32)
    out = []
    for first, size in ((0, head), (head, tail)):
        if size == 0:
            out.append(None)
            continue
        r, s = iota((n * size, n), 0), iota((n * size, n), 1)
        m = jnp.bitwise_xor(s, ep)
        mine = (r >= m * size) & (r < m * size + size)
        spread = jnp.where(mine, 1.0, 0.0)
        rank_in = jnp.sum(jnp.where(mine, r - m * size + first, 0), axis=1, keepdims=True)
        experts = jnp.sum(
            jnp.where(mine, jnp.broadcast_to(slots_row, (n * size, n)), 0), axis=1, keepdims=True
        )
        goes_r = jnp.dot(spread, goes, preferred_element_type=F32)
        place_r = jnp.dot(spread, place, preferred_element_type=F32)
        chosen = (goes_r > 0.5) & (place_r == rank_in.astype(F32))
        out.append((jnp.where(chosen, 1.0, 0.0), experts))
    return out


def kernel(n, cap, tok, ids_ref, slots_ref, gates_ref, wg_hbm, wu_hbm, wd_hbm, out_ref,
           wg, wu, wd, send_a, send_b, x_a, x_b, hid_0, hid_1, hid_2, res_a, res_b, ret_a, ret_b,
           w_sem, d_send, d_recv, s_send, s_recv, f_send, f_recv, h_send, h_recv, r_send, r_recv):
    ep, rep = lax.axis_index("ep"), lax.axis_index("rep")
    other = 1 - rep
    hid = (hid_0, hid_1, hid_2)
    rows, half = tok.shape
    tail = cap - HEAD

    barrier = pltpu.get_barrier_semaphore()

    def greet(m):
        pl.semaphore_signal(barrier, inc=1, device_id={"ep": mix(n, ep, m)}, device_id_type=MESH)

    repeat(1, n, greet)
    pl.semaphore_signal(barrier, inc=1, device_id={"rep": other}, device_id_type=MESH)

    weights = [
        pltpu.make_async_copy(wg_hbm.at[0], wg, w_sem.at[0]),
        pltpu.make_async_copy(wu_hbm.at[0], wu, w_sem.at[1]),
        pltpu.make_async_copy(
            wd_hbm.at[0, :, pl.ds(pl.multiple_of(rep * half, 128), half)], wd.at[rep], w_sem.at[2]
        ),
    ]
    for copy in weights:
        copy.start()

    (pick_a, exp_a), (pick_b, exp_b) = routing(ids_ref[...], slots_ref[...], ep, HEAD, tail)
    tokens = tok[...]
    packed = jnp.dot(pick_a.astype(BF16), tokens, preferred_element_type=F32).astype(BF16)
    send_a[...] = packed.reshape(n, HEAD, half)
    packed = jnp.dot(pick_b.astype(BF16), tokens, preferred_element_type=F32)
    for m in range(n):
        send_b[m] = packed[m * tail : m * tail + tail].astype(BF16)

    pl.semaphore_wait(barrier, n)

    def down(side):
        return pltpu.make_async_remote_copy(
            src_ref=wd_hbm.at[0, :, pl.ds(pl.multiple_of(other * half, 128), half)],
            dst_ref=wd.at[side], send_sem=d_send, recv_sem=d_recv,
            device_id={"rep": other}, device_id_type=MESH,
        )

    def packet(m, part):
        src, dst = ((send_a, x_a), (send_b, x_b))[part]
        return pltpu.make_async_remote_copy(
            src_ref=src.at[m], dst_ref=dst.at[rep, m],
            send_sem=s_send.at[part, m], recv_sem=s_recv.at[part, m],
            device_id={"ep": mix(n, ep, m)}, device_id_type=MESH,
        )

    def forward(m, part, side):
        dst = (x_a, x_b)[part]
        return pltpu.make_async_remote_copy(
            src_ref=dst.at[side, m], dst_ref=dst.at[side, m],
            send_sem=f_send.at[part, m], recv_sem=f_recv.at[part, m],
            device_id={"rep": other}, device_id_type=MESH,
        )

    def back(m, part):
        src, dst = ((res_a, ret_a), (res_b, ret_b))[part]
        return pltpu.make_async_remote_copy(
            src_ref=src.at[m], dst_ref=dst.at[m],
            send_sem=r_send.at[part, m], recv_sem=r_recv.at[part, m],
            device_id={"ep": mix(n, ep, m)}, device_id_type=MESH,
        )

    def share(b, side):
        rows_of = hid[b].at[side]
        return pltpu.make_async_remote_copy(
            src_ref=rows_of, dst_ref=rows_of, send_sem=h_send.at[b], recv_sem=h_recv.at[b],
            device_id={"rep": other}, device_id_type=MESH,
        )

    def start_packet(m):
        for part in range(2):
            packet(m, part).start()

    repeat(1, n, start_packet)
    down(rep).start()
    x_a[rep, 0] = send_a[0]
    x_b[rep, 0] = send_b[0]
    for part in range(2):
        forward(0, part, rep).start()

    mine = pl.ds(pl.multiple_of(rep * half, 16), half)
    theirs = pl.ds(pl.multiple_of(other * half, 16), half)

    for b, (lo, hi) in enumerate(batches(n)):

        def pass_on(m):
            for part in range(2):
                packet(m, part).wait_recv()
                forward(m, part, rep).start()

        def arrive(m):
            for part in range(2):
                forward(m, part, other).wait_recv()

        def block(side):
            upper = x_a[side, lo:hi].reshape((hi - lo) * HEAD, half)
            lower = x_b[side, lo:hi].reshape((hi - lo) * tail, half)
            return jnp.concatenate([upper, lower], axis=0)

        repeat(max(lo, 1), hi, pass_on)
        if b == 0:
            weights[0].wait()
            weights[1].wait()
        x_mine = block(rep)
        gate = jnp.dot(x_mine, wg[mine, :], preferred_element_type=F32)
        up = jnp.dot(x_mine, wu[mine, :], preferred_element_type=F32)
        repeat(lo, hi, arrive)
        x_theirs = block(other)
        gate = gate + jnp.dot(x_theirs, wg[theirs, :], preferred_element_type=F32)
        up = up + jnp.dot(x_theirs, wu[theirs, :], preferred_element_type=F32)
        hid[b][rep] = ((gate / (1.0 + jnp.exp(-gate))) * up).astype(BF16)
        share(b, rep).start()
        if b == 0:
            weights[2].wait()
        result = jnp.dot(hid[b][rep], wd[rep], preferred_element_type=F32)
        if b == 0:
            down(other).wait_recv()
        share(b, other).wait_recv()
        result = result + jnp.dot(hid[b][other], wd[other], preferred_element_type=F32)
        split = (hi - lo) * HEAD
        res_a[lo:hi] = result[:split].astype(BF16).reshape(hi - lo, HEAD, half)
        for m in range(lo, hi):
            at = split + (m - lo) * tail
            res_b[m] = result[at : at + tail].astype(BF16)

        def start_back(m):
            for part in range(2):
                back(m, part).start()

        repeat(max(lo, 1), hi, start_back)

    ret_a[0] = res_a[0]
    ret_b[0] = res_b[0]

    down(rep).wait_send()
    for b in range(len(batches(n))):
        share(b, rep).wait_send()

    def sent(m):
        for part in range(2):
            packet(m, part).wait_send()
            forward(m, part, rep).wait_send()

    repeat(1, n, sent)
    for part in range(2):
        forward(0, part, rep).wait_send()

    def came_back(m):
        for part in range(2):
            back(m, part).wait_recv()

    repeat(1, n, came_back)

    ids = ids_ref[...]
    gates = gates_ref[...]
    all_a = ret_a[...].reshape(n * HEAD, half)
    all_b = ret_b[...].reshape(n * tail, half)
    over = (((0,), (0,)), ((), ()))
    diagonal = iota((rows, rows), 0) == iota((rows, rows), 1)
    total = None
    for k in range(ids.shape[0]):
        hit_a = jnp.where(ids[k : k + 1, :] == exp_a, pick_a, 0.0).astype(BF16)
        hit_b = jnp.where(ids[k : k + 1, :] == exp_b, pick_b, 0.0).astype(BF16)
        got = lax.dot_general(hit_a, all_a, over, preferred_element_type=F32)
        got = got + lax.dot_general(hit_b, all_b, over, preferred_element_type=F32)
        line = jnp.broadcast_to(gates[k : k + 1, :], (rows, rows))
        column = jnp.sum(jnp.where(diagonal, line, 0.0), axis=1, keepdims=True)
        total = got * column if total is None else total + got * column
    out_ref[...] = total

    def back_sent(m):
        for part in range(2):
            back(m, part).wait_send()

    repeat(1, n, back_sent)


def batches(n):
    return ((3 * n // 4, n), (n // 2, 3 * n // 4), (0, n // 2))


def body(tokens, expert_ids, gate_values, slot_expert, gate_weight, up_weight, down_weight):
    rows, top = expert_ids.shape
    half = tokens.shape[1]
    n = slot_expert.shape[0]
    experts = n // 2
    cap = rows * top * 5 // (4 * experts)
    tail = cap - HEAD
    depth, hidden = gate_weight.shape[1:]
    vmem = pl.BlockSpec(memory_space=pltpu.VMEM)
    hbm = pl.BlockSpec(memory_space=pl.ANY)
    dma = pltpu.SemaphoreType.DMA
    combined = pl.pallas_call(
        functools.partial(kernel, n, cap),
        out_shape=jax.ShapeDtypeStruct((rows, half), F32),
        in_specs=[vmem] * 4 + [hbm] * 3,
        out_specs=vmem,
        scratch_shapes=[
            pltpu.VMEM((depth, hidden), BF16),
            pltpu.VMEM((depth, hidden), BF16),
            pltpu.VMEM((2, hidden, half), BF16),
            pltpu.VMEM((n, HEAD, half), BF16),
            pltpu.VMEM((n, tail, half), BF16),
            pltpu.VMEM((2, n, HEAD, half), BF16),
            pltpu.VMEM((2, n, tail, half), BF16),
            *(pltpu.VMEM((2, (hi - lo) * cap, hidden), BF16) for lo, hi in batches(n)),
            pltpu.VMEM((n, HEAD, half), BF16),
            pltpu.VMEM((n, tail, half), BF16),
            pltpu.VMEM((n, HEAD, half), BF16),
            pltpu.VMEM((n, tail, half), BF16),
            dma((3,)),
            dma, dma,
            dma((2, n)), dma((2, n)),
            dma((2, n)), dma((2, n)),
            dma((3,)), dma((3,)),
            dma((2, n)), dma((2, n)),
        ],
        compiler_params=pltpu.CompilerParams(
            collective_id=0, has_side_effects=True, vmem_limit_bytes=60000 * 1024
        ),
    )(tokens, expert_ids.T, slot_expert.reshape(1, n), gate_values.T,
      gate_weight, up_weight, down_weight)
    return combined.astype(BF16)


def solution(mesh):
    return jax.shard_map(
        body,
        mesh=mesh,
        in_specs=(
            P(("groups", "ep"), "rep"),
            P(("groups", "ep"), None),
            P(("groups", "ep"), None),
            P(),
            P("ep", None, "rep"),
            P("ep", None, "rep"),
            P("ep", "rep", None),
        ),
        out_specs=P(("groups", "ep"), "rep"),
        check_vma=False,
    )
```

```python
import functools

import jax
import jax.numpy as jnp
from jax import lax
from jax.experimental import pallas as pl
from jax.experimental.pallas import tpu as pltpu
from jax.sharding import PartitionSpec as P

MESH = pl.DeviceIdType.MESH
F32 = jnp.float32
BF16 = jnp.bfloat16
HEAD = 8


def iota(shape, dim):
    return lax.broadcasted_iota(jnp.int32, shape, dim)


def repeat(low, high, step):
    if high - low <= 8:
        for i in reversed(range(low, high)):
            step(i)
    else:
        lax.fori_loop(0, high - low, lambda i, c: (step(high - 1 - i), c)[1], 0)


def mix(n, a, b):
    total, bit = 0, 1
    while bit < n:
        total = total + (a // bit + b // bit) % 2 * bit
        bit *= 2
    return total


def routing(ids, slots_row, ep, tail):
    top, rows = ids.shape
    n = slots_row.shape[1]
    at_row, at_col = iota((n, n), 0), iota((n, n), 1)
    slots_all = jnp.broadcast_to(slots_row, (n, n))
    slots_col = jnp.sum(jnp.where(at_row == at_col, slots_all, 0), axis=1, keepdims=True)
    same = slots_col == slots_all
    copies = jnp.sum(jnp.where(same, 1, 0), axis=1, keepdims=True)
    rank = jnp.sum(jnp.where(same & (at_col < at_row), 1, 0), axis=1, keepdims=True)
    want = jnp.zeros_like(copies)
    for c in range(2, 5):
        want = jnp.where(copies == c, lax.rem(ep, c), want)
    goes = jnp.zeros((n, rows), F32)
    for k in range(top):
        hit = (ids[k : k + 1, :] == slots_col) & (rank == want)
        goes = jnp.where(hit, 1.0, goes)
    before = jnp.where(iota((rows, rows), 0) < iota((rows, rows), 1), 1.0, 0.0)
    place = jnp.dot(goes, before, preferred_element_type=F32)
    r, s = iota((n * HEAD, n), 0), iota((n * HEAD, n), 1)
    m = jnp.bitwise_xor(s, ep)
    mine = (r >= m * HEAD) & (r < m * HEAD + HEAD)
    spread = jnp.where(mine, 1.0, 0.0)
    index = jnp.sum(jnp.where(mine, r - m * HEAD, 0), axis=1, keepdims=True)
    experts = jnp.sum(
        jnp.where(mine, jnp.broadcast_to(slots_row, (n * HEAD, n)), 0), axis=1, keepdims=True
    )
    goes_r = jnp.dot(spread, goes, preferred_element_type=F32)
    place_r = jnp.dot(spread, place, preferred_element_type=F32)
    place_in = jnp.where(goes_r > 0.5, place_r, -1.0)
    heads = jnp.where(place_in == index.astype(F32), 1.0, 0.0)
    folds = []
    for q in range(HEAD // tail):
        wanted = jnp.where((index >= q * tail) & (index < q * tail + tail), index - q * tail + HEAD, -2)
        folds.append(jnp.where(place_in == wanted.astype(F32), 1.0, 0.0))
    return heads, folds, experts


def fold_width(half, tail):
    return (half * tail // HEAD + 127) // 128 * 128


def fold_cuts(half, tail):
    wide = fold_width(half, tail)
    return [(q * wide, min(wide, half - q * wide)) for q in range(HEAD // tail)]


def widen(piece, wide):
    short = wide - piece.shape[1]
    return jnp.concatenate([piece, jnp.zeros((piece.shape[0], short), piece.dtype)], 1) if short else piece


def kernel(n, cap, tok, ids_ref, slots_ref, gates_ref, wg_hbm, wu_hbm, wd_hbm, out_ref,
           wg, wu, wd, w_sem, d_send, d_recv, s_send, s_recv, f_send, f_recv, h_send, h_recv,
           r_send, r_recv, ready, hid, send, x, res, ret, mid, gate_mid, up_mid):
    ep, rep = lax.axis_index("ep"), lax.axis_index("rep")
    other = 1 - rep
    rows, half = tok.shape
    tail = cap - HEAD
    cuts, wide = fold_cuts(half, tail), fold_width(half, tail)

    barrier = pltpu.get_barrier_semaphore()

    width = grid_width(n)
    height = n // width
    row, col = ep // width, ep % width
    beside = (
        (row > 0, ep - width), (row < height - 1, ep + width), (col > 0, ep - 1), (col < width - 1, ep + 1),
    )
    near_count = sum(jnp.where(there, 1, 0) for there, _ in beside)

    def tell(sem):
        for there, peer in beside:

            @pl.when(there)
            def _():
                pl.semaphore_signal(sem, inc=1, device_id={"ep": peer}, device_id_type=MESH)

    tell(barrier)
    pl.semaphore_signal(barrier, inc=1, device_id={"rep": other}, device_id_type=MESH)

    weights = [
        pltpu.make_async_copy(wg_hbm.at[0], wg, w_sem.at[0]),
        pltpu.make_async_copy(wu_hbm.at[0], wu, w_sem.at[1]),
        pltpu.make_async_copy(
            wd_hbm.at[0, :, pl.ds(pl.multiple_of(rep * half, 128), half)], wd.at[rep], w_sem.at[2]
        ),
    ]
    for copy in weights:
        copy.start()

    heads, folds, experts = routing(ids_ref[...], slots_ref[...], ep, tail)
    tokens = tok[...]

    def shape_up(block):
        return block.astype(BF16).reshape(n, HEAD, block.shape[1])

    send[:, :, :half] = shape_up(jnp.dot(heads.astype(BF16), tokens, preferred_element_type=F32))
    folded = None
    for (at, size), pick in zip(cuts, folds):
        piece = jnp.dot(pick.astype(BF16), tokens[:, at : at + size], preferred_element_type=F32)
        piece = widen(piece, wide)
        folded = piece if folded is None else folded + piece
    send[:, :, half:] = shape_up(folded)

    pl.semaphore_wait(barrier, near_count + 1)

    def down(side):
        return pltpu.make_async_remote_copy(
            src_ref=wd_hbm.at[0, :, pl.ds(pl.multiple_of(other * half, 128), half)],
            dst_ref=wd.at[side], send_sem=d_send, recv_sem=d_recv,
            device_id={"rep": other}, device_id_type=MESH,
        )

    def packet(m):
        return pltpu.make_async_remote_copy(
            src_ref=send.at[m], dst_ref=x.at[rep, m],
            send_sem=s_send.at[m], recv_sem=s_recv.at[m],
            device_id={"ep": mix(n, ep, m)}, device_id_type=MESH,
        )

    def forward(m, side):
        return pltpu.make_async_remote_copy(
            src_ref=x.at[side, m], dst_ref=x.at[side, m],
            send_sem=f_send.at[m], recv_sem=f_recv.at[m],
            device_id={"rep": other}, device_id_type=MESH,
        )

    def back(m):
        return pltpu.make_async_remote_copy(
            src_ref=res.at[m], dst_ref=ret.at[m],
            send_sem=r_send.at[m], recv_sem=r_recv.at[m],
            device_id={"ep": mix(n, ep, m)}, device_id_type=MESH,
        )

    def share(side):
        return pltpu.make_async_remote_copy(
            src_ref=hid.at[side], dst_ref=hid.at[side], send_sem=h_send, recv_sem=h_recv,
            device_id={"rep": other}, device_id_type=MESH,
        )

    def start_packet(m):
        packet(m).start()

    reach = height + width - 2
    for away in range(1, reach + 1):
        if away > 1:
            pl.semaphore_wait(ready.at[away - 2], near_count)
        if away < reach:
            tell(ready.at[away - 1])
        if n <= 8:
            for m in reversed(range(1, n)):
                pl.when(steps(n, ep, m) == away)(functools.partial(start_packet, m))
    if n > 8:
        repeat(1, n, start_packet)
    down(rep).start()
    x[rep, 0] = send[0]
    forward(0, rep).start()

    def pass_on(m):
        packet(m).wait_recv()
        forward(m, rep).start()

    def tails(block):
        rows_of = [
            block[:, q * tail : q * tail + tail, :size].reshape(n * tail, size)
            for q, (_, size) in enumerate(cuts)
        ]
        return jnp.concatenate(rows_of, axis=1)

    def add(gate, up, side):
        upper = x[side, :, :, :half].reshape(n * HEAD, half)
        block = jnp.concatenate([upper, tails(x[side, :, :, half:])], axis=0)
        lines = pl.ds(pl.multiple_of(side * half, 128), half)
        g = jnp.dot(block, wg[lines, :], preferred_element_type=F32)
        u = jnp.dot(block, wu[lines, :], preferred_element_type=F32)
        return (g, u) if gate is None else (gate + g, up + u)

    for m in range(1, n):
        pass_on(m)
    weights[0].wait()
    weights[1].wait()
    gate_mid[...], up_mid[...] = add(None, None, rep)
    repeat(0, n, lambda m: forward(m, other).wait_recv())
    gate, up = add(gate_mid[...], up_mid[...], other)
    hid[rep] = ((gate / (1.0 + jnp.exp(-gate))) * up).astype(BF16)
    share(rep).start()
    weights[2].wait()
    mid[...] = jnp.dot(hid[rep], wd[rep], preferred_element_type=F32)
    down(other).wait_recv()
    share(other).wait_recv()
    result = mid[...] + jnp.dot(hid[other], wd[other], preferred_element_type=F32)
    split = n * HEAD
    res[:, :, :half] = shape_up(result[:split])
    last = result[split:].astype(BF16)
    over = (((0,), (0,)), ((), ()))
    for q, (at, size) in enumerate(cuts):
        piece = widen(last[:, at : at + size], wide).reshape(n, tail, wide)
        res[:, q * tail : q * tail + tail, half:] = piece
    repeat(1, n, lambda m: back(m).start())
    ret[0] = res[0]

    down(rep).wait_send()
    share(rep).wait_send()

    def sent(m):
        packet(m).wait_send()
        forward(m, rep).wait_send()

    repeat(1, n, sent)
    forward(0, rep).wait_send()
    repeat(1, n, lambda m: back(m).wait_recv())

    ids = ids_ref[...]
    gates = gates_ref[...]
    all_heads = ret[:, :, :half].reshape(n * HEAD, half)
    all_folds = ret[:, :, half:].reshape(n * HEAD, wide)
    diagonal = iota((rows, rows), 0) == iota((rows, rows), 1)
    total = None
    for k in range(ids.shape[0]):
        named = ids[k : k + 1, :] == experts
        hit = jnp.where(named, heads, 0.0).astype(BF16)
        got = lax.dot_general(hit, all_heads, over, preferred_element_type=F32)
        pieces = []
        for (_, size), pick in zip(cuts, folds):
            hit = jnp.where(named, pick, 0.0).astype(BF16)
            pieces.append(lax.dot_general(hit, all_folds[:, :size], over, preferred_element_type=F32))
        got = got + jnp.concatenate(pieces, axis=1)
        line = jnp.broadcast_to(gates[k : k + 1, :], (rows, rows))
        column = jnp.sum(jnp.where(diagonal, line, 0.0), axis=1, keepdims=True)
        total = got * column if total is None else total + got * column
    out_ref[...] = total

    repeat(1, n, lambda m: back(m).wait_send())


def grid_width(n):
    width = 1
    while width * width * 4 <= n:
        width *= 2
    return width


def steps(n, ep, m):
    width = grid_width(n)
    total = 0
    for here, part in ((ep // width, m // width), (ep % width, m % width)):
        top, delta = 1, 0
        while top <= part:
            delta = delta + (part // top % 2) * (1 - 2 * (here // top % 2)) * top
            top *= 2
        total = total + delta * (1 - 2 * (here // (top // 2) % 2)) if part else total
    return total


def body(tokens, expert_ids, gate_values, slot_expert, gate_weight, up_weight, down_weight):
    rows, top = expert_ids.shape
    half = tokens.shape[1]
    n = slot_expert.shape[0]
    experts = n // 2
    cap = rows * top * 5 // (4 * experts)
    tail = cap - HEAD
    depth, hidden = gate_weight.shape[1:]
    vmem = pl.BlockSpec(memory_space=pltpu.VMEM)
    hbm = pl.BlockSpec(memory_space=pl.ANY)
    dma = pltpu.SemaphoreType.DMA
    wide = half + fold_width(half, tail)

    combined = pl.pallas_call(
        functools.partial(kernel, n, cap),
        out_shape=pltpu.VMEM((rows, half), F32),
        in_specs=[vmem] * 4 + [hbm] * 3,
        out_specs=vmem,
        scratch_shapes=[
            pltpu.VMEM((depth, hidden), BF16),
            pltpu.VMEM((depth, hidden), BF16),
            pltpu.VMEM((2, hidden, half), BF16),
            dma((3,)),
            dma, dma,
            dma((n,)), dma((n,)),
            dma((n,)), dma((n,)),
            dma, dma,
            dma((n,)), dma((n,)),
            pltpu.SemaphoreType.REGULAR((max(n // grid_width(n) + grid_width(n) - 3, 1),)),
            pltpu.VMEM((2, n * cap, hidden), BF16),
            pltpu.VMEM((n, HEAD, wide), BF16),
            pltpu.VMEM((2, n, HEAD, wide), BF16),
            pltpu.VMEM((n, HEAD, wide), BF16),
            pltpu.VMEM((n, HEAD, wide), BF16),
            pltpu.VMEM((n * cap, half), F32),
            pltpu.VMEM((n * cap, hidden), F32),
            pltpu.VMEM((n * cap, hidden), F32),
        ],
        compiler_params=pltpu.CompilerParams(
            collective_id=0, has_side_effects=True, vmem_limit_bytes=60000 * 1024
        ),
    )(tokens, expert_ids.T, slot_expert.reshape(1, n), gate_values.T,
      gate_weight, up_weight, down_weight)
    return combined.astype(BF16)


def solution(mesh):
    return jax.shard_map(
        body,
        mesh=mesh,
        in_specs=(
            P(("groups", "ep"), "rep"),
            P(("groups", "ep"), None),
            P(("groups", "ep"), None),
            P(),
            P("ep", None, "rep"),
            P("ep", None, "rep"),
            P("ep", "rep", None),
        ),
        out_specs=P(("groups", "ep"), "rep"),
        check_vma=False,
    )
```
